32 devices in a mesh: fit: 16 (over z, y, x), basis: 2 (over core), occ: 1.
Axes of the slice: x: 2, y: 2, z: 4, core: 2. Of those that a mesh axis runs over, the one named last changes fastest.
Arguments:
- ints: bfloat16 [256, 12288, 128], P('fit', 'basis'), may hold values from -0.5 to 0.5
- coeffs: bfloat16 [12288, 64], P('fit', 'occ'), may hold values from -0.59765625 to 0.59765625
- offsets: int32 [192, 2], P('basis'), may hold values from 0 to 191
- mask: int32 [192, 2], P('basis'), may hold values 0 or 1
Outputs:
- exchange: float32 [12288, 4, 256], P(('fit', 'occ'), None, 'basis')
The draws below stay inside these ranges and needn't reach their ends.
All inputs are finite; a program needn't handle non-finite values. No bound on the sum of `mask` on one device may be relied on, other than what follows from the above.
Results may differ from the reference program's by a relative error of at most 0.003.
Values may be sent and summed in bfloat16 or wider, within the bound.
No kernel may reach another device: no remote copies, remote signals or barrier semaphores. Data moves between devices by JAX's collectives and lax.ppermute only.
A program may use at most 192 MiB of HBM per device.

```python
import jax
import jax.numpy as jnp
import numpy as np
from jax import lax

NB = 12288
BLK = 64
NNZ = 2
MU_DEV = 128
NAUX = 256
NOCC = 16
N_BASIS = 2


def with_ends(array, stream_key, low, high):
    longest = array.shape.index(max(array.shape))
    spots = []
    for shift in (0, 1):
        where = [jax.random.randint(jax.random.fold_in(stream_key, axis), (), 0, length) for axis, length in enumerate(array.shape)]
        where[longest] = (where[longest] + shift) % array.shape[longest]
        spots.append(tuple(where))
    return array.at[spots[0]].set(low).at[spots[1]].set(high)


def levels(stream_key, extent, cuts, smallest, largest):
    level = 1.0
    for dim, parts in cuts:
        heights = jax.random.uniform(jax.random.fold_in(jax.random.fold_in(stream_key, 6), dim), (parts,), jnp.float32, smallest / len(cuts), largest / len(cuts))
        level = level * jnp.repeat(jnp.exp(heights), extent[dim] // parts).reshape((-1,) + (1,) * (len(extent) - 1 - dim))
    return level


def noise(own_key, shape, scale, limit, shards=(), kind=jnp.bfloat16):
    gain = levels(own_key, shape, shards, -0.22, 0.18) if shards else 1.0
    result = jax.random.normal(own_key, shape, jnp.float32) * scale * gain
    return jnp.minimum(jnp.maximum(result, -limit), limit).astype(kind)


def setup_inputs(seed: int = 0) -> dict:
    streams_of = jax.random.split(jax.random.key(seed), 5)
    return {
        "ints": noise(streams_of[0], (NAUX, NB, NNZ * BLK), (NNZ * BLK) ** -0.5, 0.5, ((0, 16), (1, 2))),
        "coeffs": noise(streams_of[1], (NB, 4 * NOCC), 0.1, 0.59765625, ((0, 16),)),
        "offsets": with_ends(jax.random.randint(streams_of[2], (NB // BLK, NNZ), 0, NB // BLK), jax.random.fold_in(streams_of[2], 1), 0, (NB // BLK) - 1).astype(jnp.int32),
        "mask": with_ends((jax.random.randint(streams_of[3], (NB // BLK, NNZ), 0, 4) < 3).astype(jnp.int32), jax.random.fold_in(streams_of[3], 1), 0, 1),
    }


SIGN_ENTRIES = ((0, 0, 0, 1), (0, 1, 1, 1), (0, 2, 2, 1), (0, 3, 3, 1),
                (1, 0, 1, -1), (1, 1, 0, 1), (1, 2, 3, -1), (1, 3, 2, 1),
                (2, 0, 2, -1), (2, 1, 3, 1), (2, 2, 0, 1), (2, 3, 1, -1),
                (3, 0, 3, -1), (3, 1, 2, -1), (3, 2, 1, 1), (3, 3, 0, 1))


def sign_table():
    table = np.zeros((4, 4, 4), np.float32)
    for entry in SIGN_ENTRIES:
        table[entry[0], entry[1], entry[2]] = entry[3]
    return table


def reference(ints, coeffs, offsets, mask):
    rows_dev = NB // N_BASIS
    blocks = coeffs.reshape(NB // BLK, BLK, -1)
    picked = jnp.take(blocks, offsets, axis=0) * mask[:, :, None, None].astype(jnp.bfloat16)
    picked = picked.reshape(NB // BLK, NNZ * BLK, -1).astype(jnp.float32)
    index = jnp.arange(MU_DEV * N_BASIS, dtype=jnp.int32)
    chosen = ((index // MU_DEV) * rows_dev + index % MU_DEV).astype(jnp.int32)
    count = MU_DEV * N_BASIS
    sign = jnp.asarray(sign_table(), jnp.float32)

    def advance(total, slab):
        grouped = slab.astype(jnp.float32).reshape(NB // BLK, BLK, NNZ * BLK)
        half = jnp.einsum("rjk,rkw->rjw", grouped, picked).reshape(NB, -1).astype(jnp.bfloat16)
        window = jnp.take(half, chosen, axis=0).astype(jnp.float32).reshape(count, -1, 4)
        mixed = jnp.einsum("rqs,mkq->rmks", sign, window).reshape(4 * count, -1).astype(jnp.bfloat16)
        term = lax.dot_general(half, mixed, (((1,), (1,)), ((), ())), preferred_element_type=jnp.float32)
        return total + term, None

    total, unused = lax.scan(advance, jnp.zeros((NB, 4 * count), jnp.float32), ints)
    return total.reshape(NB, 4, count)
```

```python
import functools

import jax
import jax.numpy as jnp
import numpy as np
from jax import lax
from jax.experimental import pallas as pl
from jax.experimental.pallas import tpu as pltpu
from jax.sharding import PartitionSpec as P

BLK = 64
NNZ = 2
MU_DEV = 128
CHUNKS = (2, 2, 2)


SIGN_ENTRIES = (
    (0, 0, 0, 1),
    (0, 1, 1, 1),
    (0, 2, 2, 1),
    (0, 3, 3, 1),
    (1, 0, 1, -1),
    (1, 1, 0, 1),
    (1, 2, 3, -1),
    (1, 3, 2, 1),
    (2, 0, 2, -1),
    (2, 1, 3, 1),
    (2, 2, 0, 1),
    (2, 3, 1, -1),
    (3, 0, 3, -1),
    (3, 1, 2, -1),
    (3, 2, 1, 1),
    (3, 3, 0, 1),
)
F32 = jnp.float32
BF16 = jnp.bfloat16
LANES = 128
HEAD = 4


def mix_table():
    table = np.zeros((4, LANES, LANES), np.float32)
    for r, q, s, sign in SIGN_ENTRIES:
        for base in range(0, LANES, 4):
            table[r, base + s, base + q] = sign
    return table.reshape(4 * LANES, LANES)


def params(**more):
    return pltpu.CompilerParams(vmem_limit_bytes=40 * 1024 * 1024, **more)


def picked_pair(info, tables, row, rows, width):
    tops, bottoms = [], []
    lane = lax.broadcasted_iota(jnp.int32, (BLK, LANES), 1)
    left = lane < width
    for k in range(NNZ):
        code = info[HEAD + k * rows + row]
        safe = jnp.maximum(code, 0)
        side = jnp.bitwise_and(safe, 1)
        block = jnp.right_shift(safe, 1)
        if len(tables) == 1:
            tile = tables[0][block].astype(F32)
        else:
            part = jnp.bitwise_and(block, 1)
            block = jnp.right_shift(block, 1)
            tile = jnp.where(part == 0, tables[0][block].astype(F32), tables[1][block].astype(F32))
        tile = jnp.where(code >= 0, tile, 0.0)
        other = jnp.concatenate([tile[:, width:], tile[:, :width]], axis=1)
        low = jnp.where(side == 0, tile, other)
        high = jnp.where(side == 0, other, tile)
        tops.append(jnp.where(left, low, 0.0).astype(BF16))
        bottoms.append(jnp.where(left, 0.0, high).astype(BF16))
    return jnp.concatenate(tops + bottoms, axis=0)


def half_rows(ints, right, store):
    count, blk, stored = ints.shape
    pairs = count // 2
    lhs = jnp.concatenate(
        [ints[:pairs].reshape(pairs * blk, stored), ints[pairs:].reshape(pairs * blk, stored)], axis=1
    )
    out = jnp.dot(lhs, right, preferred_element_type=F32).astype(BF16)
    for p in range(pairs):
        store(p, out[p * blk : (p + 1) * blk])


def window_kernel(info, ints_ref, *rest, rows, width):
    *tables, out_ref = rest
    blocks = ints_ref.shape[1]
    for rb in range(blocks):
        right = picked_pair(info, tables, rb, rows, width)

        def store(p, value, rb=rb):
            out_ref[rb * BLK : (rb + 1) * BLK, p * LANES : (p + 1) * LANES] = value

        half_rows(ints_ref[:, rb], right, store)


def half_kernel(info, a_ref, b_ref, *rest, rows, width, per, first, mine):
    *tables, a_out, b_out = rest
    zl, step = pl.program_id(0), pl.program_id(1)
    x, y = info[0], info[1]
    if not mine:
        x, y = 1 - x, 1 - y
    for other in range(2):
        row_a = ((zl * 2 + other) * 2 + x) * per + first + step
        right = picked_pair(info, tables, row_a, rows, width)

        def store_a(p, value, other=other):
            a_out[0, other, 0, :, p * LANES : (p + 1) * LANES] = value

        half_rows(a_ref[:, 0, other, 0, 0], right, store_a)
        row_b = ((zl * 2 + y) * 2 + other) * per + per // 2 + first + step
        right = picked_pair(info, tables, row_b, rows, width)

        def store_b(p, value, other=other):
            b_out[0, other, 0, :, p * LANES : (p + 1) * LANES] = value

        half_rows(b_ref[:, 0, 0, other, 0], right, store_b)


def half_call(info, ints7, tables, width, first, count, mine):
    aux, zl, _, _, per, blk, stored = ints7.shape
    rows = zl * 4 * per
    depth = aux * width
    flip = 0 if mine else 1
    table_spec = pl.BlockSpec(tables[0].shape, lambda i, j, s: (0, 0, 0))
    out = jax.ShapeDtypeStruct((zl, 2, count, blk, depth), BF16)
    out_spec = pl.BlockSpec((1, 2, 1, blk, depth), lambda i, j, s: (i, 0, j, 0, 0))
    return pl.pallas_call(
        functools.partial(half_kernel, rows=rows, width=width, per=per, first=first, mine=mine),
        grid_spec=pltpu.PrefetchScalarGridSpec(
            num_scalar_prefetch=1,
            grid=(zl, count),
            in_specs=[
                pl.BlockSpec(
                    (aux, 1, 2, 1, 1, blk, stored),
                    lambda i, j, s: (0, i, 0, jnp.bitwise_xor(s[0], flip), first + j, 0, 0),
                ),
                pl.BlockSpec(
                    (aux, 1, 1, 2, 1, blk, stored),
                    lambda i, j, s: (0, i, jnp.bitwise_xor(s[1], flip), 0, per // 2 + first + j, 0, 0),
                ),
            ]
            + [table_spec] * len(tables),
            out_specs=[out_spec, out_spec],
        ),
        out_shape=[out, out],
        compiler_params=params(),
        cost_estimate=pl.CostEstimate(
            flops=4 * zl * count * aux * blk * stored * LANES * 4,
            bytes_accessed=4 * zl * count * aux * blk * (stored + width) * 2,
            transcendentals=0,
        ),
        name="half_keep" if mine else "half_send",
    )(info, ints7, ints7, *tables)


def mix_kernel(info, table_ref, *rest, parts):
    *windows, out_ref = rest
    b = info[3]
    depth = out_ref.shape[2]
    for shift in range(parts):
        slot = lax.rem(b - shift + parts, parts)
        for t in range(depth // LANES):
            tile = windows[shift][0, :, t * LANES : (t + 1) * LANES]
            mixed = lax.dot_general(
                table_ref[...], tile, (((1,), (1,)), ((), ())), preferred_element_type=F32
            ).astype(BF16)
            for r in range(4):
                out_ref[0, slot, t * LANES : (t + 1) * LANES, r * MU_DEV : (r + 1) * MU_DEV] = mixed[
                    r * LANES : (r + 1) * LANES
                ]


def send_kernel(info, ak_ref, ar_ref, bk_ref, br_ref, mix_ref, a_out, b_out):
    rows = ak_ref.shape[0] * ak_ref.shape[2] * BLK
    depth = ak_ref.shape[4]
    for own, got, k, out in ((ak_ref, ar_ref, 1, a_out), (bk_ref, br_ref, 2, b_out)):
        total = jnp.dot(own[...].reshape(rows, depth), mix_ref[0, 0], preferred_element_type=F32)
        total += jnp.dot(got[...].reshape(rows, depth), mix_ref[k, 0], preferred_element_type=F32)
        out[...] = total.astype(BF16).reshape(out.shape)


def send_call(info, a_keep, a_got, b_keep, b_got, mix):
    zl, _, count, blk, depth = a_keep.shape
    _, parts, _, cols = mix.shape
    a_spec = pl.BlockSpec((zl, 1, count, blk, depth), lambda j, s: (0, 1 - s[1], 0, 0, 0))
    b_spec = pl.BlockSpec((zl, 1, count, blk, depth), lambda j, s: (0, 1 - s[0], 0, 0, 0))
    out = jax.ShapeDtypeStruct((zl, count, blk, parts * cols), BF16)
    out_spec = pl.BlockSpec((zl, count, blk, cols), lambda j, s: (0, 0, 0, j))
    return pl.pallas_call(
        send_kernel,
        grid_spec=pltpu.PrefetchScalarGridSpec(
            num_scalar_prefetch=1,
            grid=(parts,),
            in_specs=[a_spec, a_spec, b_spec, b_spec, pl.BlockSpec((3, 1, depth, cols), lambda j, s: (0, j, 0, 0))],
            out_specs=[out_spec, out_spec],
        ),
        out_shape=[out, out],
        compiler_params=params(),
        cost_estimate=pl.CostEstimate(
            flops=2 * 4 * zl * count * blk * depth * parts * cols,
            bytes_accessed=2 * (4 * zl * count * blk * depth + 3 * depth * parts * cols),
            transcendentals=0,
        ),
        name="send_sums",
    )(info, a_keep, a_got, b_keep, b_got, mix)


def keep_kernel(info, ak_ref, ar_ref, bk_ref, br_ref, ac_ref, bc_ref, mix_ref, *outs, order):
    step = pl.program_id(0)
    rows = ak_ref.shape[2] * BLK
    depth = ak_ref.shape[4]
    totals = []
    for own, got, add, k in ((ak_ref, ar_ref, ac_ref, 1), (bk_ref, br_ref, bc_ref, 2)):
        total = jnp.dot(own[...].reshape(rows, depth), mix_ref[0, 0], preferred_element_type=F32)
        total += jnp.dot(got[...].reshape(rows, depth), mix_ref[k, 0], preferred_element_type=F32)
        total += add[...].astype(F32).reshape(total.shape)
        totals.append(total.astype(BF16).reshape(outs[0].shape[1:]))
    for place, k in enumerate(order):

        @pl.when(step == place)
        def _():
            outs[k][0] = totals[0]
            outs[k][1] = totals[1]


def keep_call(info, a_keep, a_got, b_keep, b_got, a_sum, b_sum, mix, hops):
    zl, _, count, blk, depth = a_keep.shape
    _, parts, _, cols = mix.shape
    order = [(i % zl) * parts + i // zl for i in range(hops)]

    def chosen(i, s):
        return jnp.bitwise_xor(s[2], lax.rem(i, zl) * parts + lax.div(i, zl))

    def group(i, s):
        return lax.div(chosen(i, s), parts)

    def place(i, s):
        return lax.rem(chosen(i, s), parts)

    a_spec = pl.BlockSpec((1, 1, count, blk, depth), lambda i, s: (group(i, s), s[1], 0, 0, 0))
    b_spec = pl.BlockSpec((1, 1, count, blk, depth), lambda i, s: (group(i, s), s[0], 0, 0, 0))
    sum_spec = pl.BlockSpec((1, count, blk, cols), lambda i, s: (group(i, s), 0, 0, place(i, s)))
    mix_spec = pl.BlockSpec((3, 1, depth, cols), lambda i, s: (0, place(i, s), 0, 0))
    out = jax.ShapeDtypeStruct((2, count, blk, cols), BF16)
    out_spec = pl.BlockSpec((2, count, blk, cols), lambda i, s: (0, 0, 0, 0))
    return pl.pallas_call(
        functools.partial(keep_kernel, order=order),
        grid_spec=pltpu.PrefetchScalarGridSpec(
            num_scalar_prefetch=1,
            grid=(hops,),
            in_specs=[a_spec, a_spec, b_spec, b_spec, sum_spec, sum_spec, mix_spec],
            out_specs=[out_spec] * hops,
        ),
        out_shape=[out] * hops,
        compiler_params=params(),
        cost_estimate=pl.CostEstimate(
            flops=2 * 4 * zl * count * blk * depth * parts * cols,
            bytes_accessed=2 * (4 * zl * count * blk * depth + 3 * depth * parts * cols),
            transcendentals=0,
        ),
        name="keep_sums",
    )(info, a_keep, a_got, b_keep, b_got, a_sum, b_sum, mix)


def final_kernel(*refs, chunks, hops):
    out_ref = refs[-1]
    half = out_ref.shape[0] // 2
    first = 0
    for n, count in enumerate(chunks):
        for color in range(2):
            for rb in range(count):
                total = refs[n * hops][color, rb].astype(F32)
                for k in range(1, hops):
                    total += refs[n * hops + k][color, rb].astype(F32)
                for r in range(4):
                    out_ref[color * half + first + rb, :, r, :] = total[:, r * MU_DEV : (r + 1) * MU_DEV]
        first += count


def shards(ints, coeffs, offsets, mask, *, fit, parts):
    aux, rows, stored = ints.shape
    local, width = coeffs.shape
    hops = fit // 4
    zl = fit // (4 * parts)
    owned = local // BLK
    row_blocks = rows // BLK
    per = row_blocks // (4 * zl)
    half = owned // 2
    split = 2 if parts == 2 and half % 2 == 0 else 1

    f = lax.axis_index("fit").astype(jnp.int32)
    b = lax.axis_index("basis").astype(jnp.int32)
    x, y, z = f & 1, (f >> 1) & 1, f >> 2

    def over(pattern):
        return [(i, pattern(i)) for i in range(fit)]

    def hop_x(value):
        return lax.ppermute(value, "fit", over(lambda i: i ^ 1))

    def hop_y(value):
        return lax.ppermute(value, "fit", over(lambda i: i ^ 2))

    def across(value, shift):
        return lax.ppermute(value, "basis", [(i, (i + shift) % parts) for i in range(parts)])

    table = jnp.concatenate([coeffs[: local // 2], coeffs[local // 2 :]], axis=1)
    if split == 2:
        table = lax.dynamic_slice_in_dim(table, b * (local // 4), local // 4, 0)
    table = jnp.stack([table] + [lax.ppermute(table, "fit", over(lambda i, s=s: i ^ (4 * s))) for s in range(1, hops)])
    table = jnp.stack([table] + [lax.ppermute(table, "fit", over(lambda i, s=s: i ^ s)) for s in range(1, 4)])
    tables = [table.reshape(-1, BLK, 2 * width)]
    if split == 2:
        tables.append(across(tables[0], 1))

    source, inner = offsets // owned, offsets % owned
    side, inner = inner // half, inner % half
    share = half // split
    code = ((source & 3) ^ (f & 3)) * hops + ((source >> 2) ^ z)
    code = code * share + inner % share
    if split == 2:
        code = code * 2 + ((inner // share) ^ b)
    code = jnp.where(mask != 0, code * 2 + side, -1)
    info = jnp.concatenate([jnp.stack([x, y, z, b]), code.T.reshape(-1)])

    ints7 = ints.reshape(aux, zl, 2, 2, per, BLK, stored)
    depth = aux * width
    whole = pl.BlockSpec(memory_space=pltpu.VMEM)
    window_blocks = MU_DEV // BLK
    window = pl.pallas_call(
        functools.partial(window_kernel, rows=row_blocks, width=width),
        grid_spec=pltpu.PrefetchScalarGridSpec(
            num_scalar_prefetch=1,
            grid=(1,),
            in_specs=[pl.BlockSpec((aux, window_blocks, BLK, stored), lambda i, s: (0, 0, 0, 0))]
            + [pl.BlockSpec(tables[0].shape, lambda i, s: (0, 0, 0))] * len(tables),
            out_specs=pl.BlockSpec((MU_DEV, depth), lambda i, s: (0, 0)),
        ),
        out_shape=jax.ShapeDtypeStruct((MU_DEV, depth), BF16),
        compiler_params=params(),
        cost_estimate=pl.CostEstimate(flops=2 * MU_DEV * depth * stored, bytes_accessed=2 * MU_DEV * depth * 4, transcendentals=0),
        name="window",
    )(info, ints.reshape(aux, row_blocks, BLK, stored), *tables)
    windows = jnp.stack([window, hop_x(window), hop_y(window)])
    windows = [windows] + [across(windows, s) for s in range(1, parts)]

    firsts = [sum(CHUNKS[:n]) for n in range(len(CHUNKS))] if sum(CHUNKS) * 2 == per else [0]
    counts = list(CHUNKS) if len(firsts) > 1 else [per // 2]
    keeps, gots = [], []
    for first, count in zip(firsts, counts):
        a_send, b_send = half_call(info, ints7, tables, width, first, count, False)
        gots.append((hop_x(a_send), hop_y(b_send)))
        keeps.append(half_call(info, ints7, tables, width, first, count, True))

    cols = 4 * MU_DEV
    window_spec = pl.BlockSpec((1, MU_DEV, depth), lambda i, s: (i, 0, 0))
    mix = pl.pallas_call(
        functools.partial(mix_kernel, parts=parts),
        grid_spec=pltpu.PrefetchScalarGridSpec(
            num_scalar_prefetch=1,
            grid=(3,),
            in_specs=[pl.BlockSpec((4 * LANES, LANES), lambda i, s: (0, 0))] + [window_spec] * parts,
            out_specs=pl.BlockSpec((1, parts, depth, cols), lambda i, s: (i, 0, 0, 0)),
        ),
        out_shape=jax.ShapeDtypeStruct((3, parts, depth, cols), BF16),
        compiler_params=params(),
        cost_estimate=pl.CostEstimate(
            flops=2 * 3 * parts * depth * cols * LANES, bytes_accessed=2 * 3 * parts * depth * cols, transcendentals=0
        ),
        name="mix",
    )(info, jnp.asarray(mix_table(), BF16), *windows)

    final = []
    for (a_keep, b_keep), (a_got, b_got) in zip(keeps, gots):
        a_sum, b_sum = send_call(info, a_keep, a_got, b_keep, b_got, mix)
        a_sum, b_sum = hop_y(a_sum), hop_x(b_sum)
        outs = keep_call(info, a_keep, a_got, b_keep, b_got, a_sum, b_sum, mix, hops)
        for k, value in enumerate(outs):
            pairs = []
            for i in range(fit):
                for core in range(parts):
                    goal = core * hops + ((i >> 2) ^ k)
                    pairs.append((i * parts + core, ((goal // parts) * 4 + (i & 3)) * parts + goal % parts))
            final.append(lax.ppermute(value, ("fit", "basis"), pairs))

    result = pl.pallas_call(
        functools.partial(final_kernel, chunks=counts, hops=hops),
        in_specs=[whole] * len(final),
        out_specs=whole,
        out_shape=jax.ShapeDtypeStruct((per, BLK, 4, MU_DEV), F32),
        compiler_params=params(),
        cost_estimate=pl.CostEstimate(flops=hops * per * BLK * cols, bytes_accessed=(2 * hops + 4) * per * BLK * cols, transcendentals=0),
        name="final",
    )(*final)
    result = result.reshape(per * BLK, 4, MU_DEV)
    if lax.axis_size("occ") > 1:
        result = lax.psum_scatter(result, "occ", scatter_dimension=0, tiled=True)
    return result


def solution(mesh):
    return jax.shard_map(
        functools.partial(shards, fit=mesh.shape["fit"], parts=mesh.shape["basis"]),
        mesh=mesh,
        in_specs=(P("fit", "basis", None), P("fit", "occ"), P("basis", None), P("basis", None)),
        out_specs=P(("fit", "occ"), None, "basis"),
        check_vma=False,
    )
```

```python
import functools

import jax
import jax.numpy as jnp
import numpy as np
from jax import lax
from jax.experimental import pallas as pl
from jax.experimental.pallas import tpu as pltpu
from jax.sharding import PartitionSpec as P


BLK = 64
NNZ = 2
MU_DEV = 128
CHUNKS = (2, 1, 2, 1)


SIGN_ENTRIES = (
    (0, 0, 0, 1),
    (0, 1, 1, 1),
    (0, 2, 2, 1),
    (0, 3, 3, 1),
    (1, 0, 1, -1),
    (1, 1, 0, 1),
    (1, 2, 3, -1),
    (1, 3, 2, 1),
    (2, 0, 2, -1),
    (2, 1, 3, 1),
    (2, 2, 0, 1),
    (2, 3, 1, -1),
    (3, 0, 3, -1),
    (3, 1, 2, -1),
    (3, 2, 1, 1),
    (3, 3, 0, 1),
)
F32 = jnp.float32
BF16 = jnp.bfloat16
LANES = 128
HEAD = 4


def mix_table():
    table = np.zeros((4, LANES, LANES), np.float32)
    for r, q, s, sign in SIGN_ENTRIES:
        for base in range(0, LANES, 4):
            table[r, base + s, base + q] = sign
    return table.reshape(4 * LANES, LANES)


def params(mebibytes=16):
    return pltpu.CompilerParams(vmem_limit_bytes=mebibytes * 1024 * 1024)


def picked_pair(info, tables, row, rows, width):
    tops, bottoms = [], []
    lane = lax.broadcasted_iota(jnp.int32, (BLK, LANES), 1)
    left = lane < width
    for k in range(NNZ):
        code = info[HEAD + k * rows + row]
        safe = jnp.maximum(code, 0)
        side = jnp.bitwise_and(safe, 1)
        block = jnp.right_shift(safe, 1)
        if len(tables) == 1:
            tile = tables[0][block].astype(F32)
        else:
            part = jnp.bitwise_and(block, 1)
            block = jnp.right_shift(block, 1)
            tile = jnp.where(part == 0, tables[0][block].astype(F32), tables[1][block].astype(F32))
        tile = jnp.where(code >= 0, tile, 0.0)
        other = jnp.concatenate([tile[:, width:], tile[:, :width]], axis=1)
        low = jnp.where(side == 0, tile, other)
        high = jnp.where(side == 0, other, tile)
        tops.append(jnp.where(left, low, 0.0).astype(BF16))
        bottoms.append(jnp.where(left, 0.0, high).astype(BF16))
    return jnp.concatenate(tops + bottoms, axis=0)


def half_rows(ints, right):
    count, blk, stored = ints.shape
    pairs = count // 2
    lhs = jnp.concatenate(
        [ints[:pairs].reshape(pairs * blk, stored), ints[pairs:].reshape(pairs * blk, stored)], axis=1
    )
    return jnp.dot(lhs, right, preferred_element_type=F32).astype(BF16)


def window_kernel(info, ints_ref, *rest, rows, width):
    *tables, out_ref = rest
    for rb in range(ints_ref.shape[1]):
        value = half_rows(ints_ref[:, rb], picked_pair(info, tables, rb, rows, width))
        for p in range(value.shape[0] // BLK):
            out_ref[rb * BLK : (rb + 1) * BLK, p * LANES : (p + 1) * LANES] = value[p * BLK : (p + 1) * BLK]


def half_kernel(info, a_ref, b_ref, *rest, rows, width, per, first):
    *tables, a_out, b_out = rest
    zl, step = pl.program_id(0), first + pl.program_id(1)
    color_rows(info, a_ref, b_ref, tables, zl, step, 1 - info[0], 1 - info[1], rows, width, per, [a_out], [b_out], [None])


def color_rows(info, a_ref, b_ref, tables, zl, step, x, y, rows, width, per, a_outs, b_outs, tests):
    for other in range(2):
        for ref, outs, row in (
            (a_ref, a_outs, ((zl * 2 + other) * 2 + x) * per + step),
            (b_ref, b_outs, ((zl * 2 + y) * 2 + other) * per + per // 2 + step),
        ):
            right = picked_pair(info, tables, row, rows, width)
            ints = ref[:, 0, other, 0, 0] if ref is a_ref else ref[:, 0, 0, other, 0]
            value = half_rows(ints, right)
            for out, test in zip(outs, tests):

                def store(out=out, other=other, value=value):
                    for p in range(value.shape[0] // BLK):
                        out[0, other, 0, :, p * LANES : (p + 1) * LANES] = value[p * BLK : (p + 1) * BLK]

                if test is None:
                    store()
                else:
                    pl.when(test)(store)


def rest_kernel(info, a_ref, b_ref, a_far, b_far, *rest, rows, width, per, firsts, counts, parts):
    tables, outs = rest[:parts], rest[parts:]
    zl, step = pl.program_id(0), pl.program_id(1)
    color_rows(info, a_ref, b_ref, tables, zl, step, info[0], info[1], rows, width, per, outs[:1], outs[1:2], [None])
    if counts:

        @pl.when(step >= firsts[0])
        def _():
            tests = [jnp.logical_and(step >= f, step < f + c) for f, c in zip(firsts, counts)]
            color_rows(
                info, a_far, b_far, tables, zl, step, 1 - info[0], 1 - info[1], rows, width, per, outs[2::2], outs[3::2], tests
            )


def half_specs(ints7, flip, shift, least):
    aux, _, _, _, per, blk, stored = ints7.shape
    return [
        pl.BlockSpec(
            (aux, 1, 2, 1, 1, blk, stored),
            lambda i, j, s: (0, i, 0, jnp.bitwise_xor(s[0], flip), jnp.maximum(shift + j, least), 0, 0),
        ),
        pl.BlockSpec(
            (aux, 1, 1, 2, 1, blk, stored),
            lambda i, j, s: (0, i, jnp.bitwise_xor(s[1], flip), 0, per // 2 + jnp.maximum(shift + j, least), 0, 0),
        ),
    ]


def half_call(info, ints7, tables, width, firsts, counts, name):
    aux, zl, _, _, per, blk, stored = ints7.shape
    keep = name == "half_rest"
    steps = per // 2 if keep else counts[0]
    shapes, specs = [], []
    for first, count in [(0, steps)] + list(zip(firsts, counts)) if keep else [(0, steps)]:
        shapes += [jax.ShapeDtypeStruct((zl, 2, count, blk, aux * width), BF16)] * 2
        specs += [
            pl.BlockSpec(
                (1, 2, 1, blk, aux * width),
                lambda i, j, s, first=first, count=count: (i, 0, jnp.clip(j - first, 0, count - 1), 0, 0),
            )
        ] * 2
    common = dict(rows=zl * 4 * per, width=width, per=per)
    if keep:
        least = firsts[0] if firsts else 0
        inputs = half_specs(ints7, 0, 0, 0) + half_specs(ints7, 1, 0, least)
        kernel = functools.partial(rest_kernel, firsts=firsts, counts=counts, parts=len(tables), **common)
    else:
        inputs = half_specs(ints7, 1, firsts[0], 0)
        kernel = functools.partial(half_kernel, first=firsts[0], **common)
    work = 4 * zl * (sum(counts) + (steps if keep else 0)) * aux * blk
    return pl.pallas_call(
        kernel,
        grid_spec=pltpu.PrefetchScalarGridSpec(
            num_scalar_prefetch=1,
            grid=(zl, steps),
            in_specs=inputs + [pl.BlockSpec(tables[0].shape, lambda i, j, s: (0, 0, 0))] * len(tables),
            out_specs=specs,
        ),
        out_shape=shapes,
        compiler_params=params(40),
        cost_estimate=pl.CostEstimate(
            flops=work * stored * LANES * 8, bytes_accessed=work * (stored + width) * 2, transcendentals=0
        ),
    )(info, *([ints7] * len(inputs)), *tables)


def mix_kernel(info, table_ref, *rest, parts):
    *windows, out_ref = rest
    b = info[3]
    depth = out_ref.shape[2]
    for shift in range(parts):
        slot = lax.rem(b - shift + parts, parts)
        for t in range(depth // LANES):
            tile = windows[shift][0, :, t * LANES : (t + 1) * LANES]
            mixed = lax.dot_general(
                table_ref[...], tile, (((1,), (1,)), ((), ())), preferred_element_type=F32
            ).astype(BF16)
            for r in range(4):
                out_ref[0, slot, t * LANES : (t + 1) * LANES, r * MU_DEV : (r + 1) * MU_DEV] = mixed[
                    r * LANES : (r + 1) * LANES
                ]


def both_sums(refs, mix_ref, place, count):
    a_own, b_own, a_got, b_got = refs[:count], refs[count : 2 * count], refs[2 * count], refs[2 * count + 1]
    zl, depth = a_own[0].shape[0], a_own[0].shape[4]
    rows = zl * count * BLK
    own = [ref[:, 0] for ref in a_own], [ref[:, 0] for ref in b_own]
    own = [jnp.concatenate(pieces, axis=1).reshape(rows, depth) for pieces in own]
    both = jnp.dot(jnp.concatenate(own, axis=0), mix_ref[0, place], preferred_element_type=F32)
    sums = []
    for n, got in enumerate((a_got, b_got)):
        more = jnp.dot(got[...].reshape(rows, depth), mix_ref[n + 1, place], preferred_element_type=F32)
        sums.append(both[n * rows : (n + 1) * rows] + more)
    return sums


def send_kernel(info, *refs, count):
    *refs, mix_ref, a_out, b_out = refs
    cols = mix_ref.shape[3]
    for place in range(mix_ref.shape[1]):
        for total, out in zip(both_sums(refs, mix_ref, place, count), (a_out, b_out)):
            out[:, :, :, place * cols : (place + 1) * cols] = total.astype(BF16).reshape(out.shape[:3] + (cols,))


def keep_kernel(info, *refs, count, hops):
    refs, outs = refs[:-hops], refs[-hops:]
    *refs, a_add, b_add, mix_ref = refs
    parts, cols = mix_ref.shape[1], mix_ref.shape[3]
    zl = hops // parts
    for place in range(parts):
        sums = both_sums(refs, mix_ref, place, count)
        for color, add in enumerate((a_add, b_add)):
            more = add[:, :, :, place * cols : (place + 1) * cols].astype(F32)
            sums[color] = (sums[color].reshape(more.shape) + more).astype(BF16)
        for group in range(zl):
            k = jnp.bitwise_xor(info[2], group * parts + place)
            for hop in range(hops):

                @pl.when(k == hop)
                def _(hop=hop, group=group, sums=sums):
                    for color in range(2):
                        outs[hop][color] = sums[color][group]


def sums_call(info, keep, got, mix, first, count, hops, adds=None):
    (a_keep, b_keep), (a_got, b_got) = keep, got
    zl, _, _, blk, depth = a_keep.shape
    _, parts, _, cols = mix.shape
    flip = 1 if adds is None else 0

    def own(axis):
        return [
            pl.BlockSpec((zl, 1, 1, blk, depth), lambda i, s, n=n: (0, jnp.bitwise_xor(s[axis], flip), first + n, 0, 0))
            for n in range(count)
        ]

    def other(axis):
        return [pl.BlockSpec((zl, 1, count, blk, depth), lambda i, s: (0, jnp.bitwise_xor(s[axis], flip), 0, 0, 0))]

    specs = own(1) + own(0) + other(1) + other(0)
    operands = [a_keep] * count + [b_keep] * count + [a_got, b_got]
    if adds is not None:
        specs += [pl.BlockSpec((zl, count, blk, parts * cols), lambda i, s: (0, 0, 0, 0))] * 2
        operands += list(adds)
    specs += [pl.BlockSpec(mix.shape, lambda i, s: (0, 0, 0, 0))]
    if adds is None:
        kernel = functools.partial(send_kernel, count=count)
        outs = [jax.ShapeDtypeStruct((zl, count, blk, parts * cols), BF16)] * 2
    else:
        kernel = functools.partial(keep_kernel, count=count, hops=hops)
        outs = [jax.ShapeDtypeStruct((2, count, blk, cols), BF16)] * hops
    return pl.pallas_call(
        kernel,
        grid_spec=pltpu.PrefetchScalarGridSpec(
            num_scalar_prefetch=1,
            grid=(1,),
            in_specs=specs,
            out_specs=[pl.BlockSpec(o.shape, lambda i, s: (0, 0, 0, 0)) for o in outs],
        ),
        out_shape=outs,
        compiler_params=params(),
        cost_estimate=pl.CostEstimate(
            flops=2 * 4 * zl * count * blk * depth * parts * cols,
            bytes_accessed=2 * (4 * zl * count * blk * depth + 3 * depth * parts * cols),
            transcendentals=0,
        ),
        name="send_sums" if adds is None else "keep_sums",
    )(info, *operands, mix)


def final_kernel(*refs, starts, counts, hops):
    out_ref = refs[-1]
    half = out_ref.shape[0] // 2
    for n, (first, count) in enumerate(zip(starts, counts)):
        for color in range(2):
            for rb in range(count):
                total = refs[n * hops][color, rb].astype(F32)
                for k in range(1, hops):
                    total += refs[n * hops + k][color, rb].astype(F32)
                row = color * half + first + rb
                for r in range(4):
                    out_ref[row, :, r, :] = total[:, r * MU_DEV : (r + 1) * MU_DEV]


def last_kernel(*refs, count, hops):
    out_ref = refs[-1]
    color = pl.program_id(0)
    for rb in range(count):
        total = refs[0][color, rb].astype(F32)
        for k in range(1, hops):
            total += refs[k][color, rb].astype(F32)
        for r in range(4):
            out_ref[rb, :, r, :] = total[:, r * MU_DEV : (r + 1) * MU_DEV]


def shards(ints, coeffs, offsets, mask, *, fit, parts):
    aux, rows, stored = ints.shape
    local, width = coeffs.shape
    hops = fit // 4
    zl = fit // (4 * parts)
    owned = local // BLK
    row_blocks = rows // BLK
    per = row_blocks // (4 * zl)
    half = owned // 2
    split = 2 if parts == 2 and half % 2 == 0 else 1

    f = lax.axis_index("fit").astype(jnp.int32)
    b = lax.axis_index("basis").astype(jnp.int32)
    x, y, z = f & 1, (f >> 1) & 1, f >> 2

    def over(pattern):
        return [(i, pattern(i)) for i in range(fit)]

    def hop_x(value):
        return lax.ppermute(value, "fit", over(lambda i: i ^ 1))

    def hop_y(value):
        return lax.ppermute(value, "fit", over(lambda i: i ^ 2))

    def across(value, shift):
        return lax.ppermute(value, "basis", [(i, (i + shift) % parts) for i in range(parts)])

    table = jnp.concatenate([coeffs[: local // 2], coeffs[local // 2 :]], axis=1)
    if split == 2:
        table = lax.dynamic_slice_in_dim(table, b * (local // 4), local // 4, 0)

    def spread(value, along):
        def goal(i, core, s):
            plane = along if split == 1 else along ^ (core == 1)
            return i ^ s if plane else i ^ (4 * s)

        return [
            lax.ppermute(
                value, ("fit", "basis"), [(i * parts + c, goal(i, c, s) * parts + c) for i in range(fit) for c in range(parts)]
            )
            for s in range(1, hops)
        ]

    even = hops == 4
    if even:
        table = jnp.stack([table] + spread(table, False))
        table = jnp.stack([table] + spread(table, True))
    else:
        table = lax.all_gather(table, "fit", axis=0)
    tables = [table.reshape(-1, BLK, 2 * width)]
    if split == 2:
        tables.append(across(tables[0], 1))

    source, inner = offsets // owned, offsets % owned
    side, inner = inner // half, inner % half
    share = half // split
    near, far = (source & 3) ^ (f & 3), (source >> 2) ^ z
    if not even:
        code = source
    elif split == 2:
        code = jnp.where(inner // share == 0, near * hops + far, far * 4 + near)
    else:
        code = near * hops + far
    code = code * share + inner % share
    if split == 2:
        code = code * 2 + ((inner // share) ^ b)
    code = jnp.where(mask != 0, code * 2 + side, -1)
    info = jnp.concatenate([jnp.stack([x, y, z, b]), code.T.reshape(-1)])

    ints7 = ints.reshape(aux, zl, 2, 2, per, BLK, stored)
    depth = aux * width
    whole = pl.BlockSpec(memory_space=pltpu.VMEM)
    window_blocks = MU_DEV // BLK
    window_call = pl.pallas_call(
        functools.partial(window_kernel, rows=row_blocks, width=width),
        grid_spec=pltpu.PrefetchScalarGridSpec(
            num_scalar_prefetch=1,
            grid=(1,),
            in_specs=[pl.BlockSpec((aux, window_blocks, BLK, stored), lambda i, s: (0, 0, 0, 0))]
            + [pl.BlockSpec(tables[0].shape, lambda i, s: (0, 0, 0))] * len(tables),
            out_specs=pl.BlockSpec((MU_DEV, depth), lambda i, s: (0, 0)),
        ),
        out_shape=jax.ShapeDtypeStruct((MU_DEV, depth), BF16),
        compiler_params=params(40),
        cost_estimate=pl.CostEstimate(
            flops=2 * MU_DEV * depth * stored, bytes_accessed=2 * MU_DEV * depth * 4, transcendentals=0
        ),
        name="window",
    )
    window = window_call(info, ints.reshape(aux, row_blocks, BLK, stored), *tables)
    wx, wy = hop_x(window), hop_y(window)

    firsts = [sum(CHUNKS[:n]) for n in range(len(CHUNKS))]
    counts = list(CHUNKS)
    sends = []
    for n in range(2):
        sends += half_call(info, ints7, tables, width, firsts[n : n + 1], counts[n : n + 1], f"half_{n}")
    a_keep, b_keep, *more = half_call(info, ints7, tables, width, firsts[2:], counts[2:], "half_rest")
    sends += more
    gots = [(hop_x(sends[2 * n]), hop_y(sends[2 * n + 1])) for n in range(len(counts))]

    windows = jnp.stack([window, wx, wy])
    windows = [windows] + [across(windows, s) for s in range(1, parts)]

    cols = 4 * MU_DEV
    window_spec = pl.BlockSpec((1, MU_DEV, depth), lambda i, s: (i, 0, 0))
    mix_call = pl.pallas_call(
        functools.partial(mix_kernel, parts=parts),
        grid_spec=pltpu.PrefetchScalarGridSpec(
            num_scalar_prefetch=1,
            grid=(3,),
            in_specs=[pl.BlockSpec((4 * LANES, LANES), lambda i, s: (0, 0))] + [window_spec] * parts,
            out_specs=pl.BlockSpec((1, parts, depth, cols), lambda i, s: (i, 0, 0, 0)),
        ),
        out_shape=jax.ShapeDtypeStruct((3, parts, depth, cols), BF16),
        compiler_params=params(),
        cost_estimate=pl.CostEstimate(
            flops=2 * 3 * parts * depth * cols * LANES, bytes_accessed=2 * 3 * parts * depth * cols, transcendentals=0
        ),
        name="mix",
    )
    mix = mix_call(info, jnp.asarray(mix_table(), BF16), *windows)

    final = []
    for n, got in enumerate(gots):
        a_sum, b_sum = sums_call(info, (a_keep, b_keep), got, mix, firsts[n], counts[n], hops)
        adds = hop_y(a_sum), hop_x(b_sum)
        outs = sums_call(info, (a_keep, b_keep), got, mix, firsts[n], counts[n], hops, adds)
        for k, value in enumerate(outs):
            pairs = []
            for i in range(fit):
                for core in range(parts):
                    goal = core * hops + ((i >> 2) ^ k)
                    pairs.append((i * parts + core, ((goal // parts) * 4 + (i & 3)) * parts + goal % parts))
            final.append(lax.ppermute(value, ("fit", "basis"), pairs))

    shape = jax.ShapeDtypeStruct((per, BLK, 4, MU_DEV), F32)
    early = pl.pallas_call(
        functools.partial(final_kernel, starts=firsts[:-1], counts=counts[:-1], hops=hops),
        in_specs=[whole] * len(final[:-hops]),
        out_specs=whole,
        out_shape=shape,
        compiler_params=params(),
        cost_estimate=pl.CostEstimate(
            flops=hops * per * BLK * cols, bytes_accessed=(2 * hops + 4) * per * BLK * cols, transcendentals=0
        ),
        name="early",
    )(*final[:-hops])
    last = counts[-1]
    result = pl.pallas_call(
        functools.partial(last_kernel, count=last, hops=hops),
        grid=(2,),
        in_specs=[pl.BlockSpec(final[-1].shape, lambda i: (0, 0, 0, 0))] * hops + [pl.BlockSpec(memory_space=pl.ANY)],
        out_specs=pl.BlockSpec((last, BLK, 4, MU_DEV), lambda i: ((i + 1) * (per // (2 * last)) - 1, 0, 0, 0)),
        out_shape=shape,
        input_output_aliases={hops: 0},
        compiler_params=params(),
        name="last",
    )(*final[-hops:], early)
    result = result.reshape(per * BLK, 4, MU_DEV)
    if lax.axis_size("occ") > 1:
        result = lax.psum_scatter(result, "occ", scatter_dimension=0, tiled=True)
    return result


def solution(mesh):
    def body(*args):
        return shards(*args, fit=mesh.shape["fit"], parts=mesh.shape["basis"])

    return jax.shard_map(
        body,
        mesh=mesh,
        in_specs=(P("fit", "basis", None), P("fit", "occ"), P("basis", None), P("basis", None)),
        out_specs=P(("fit", "occ"), None, "basis"),
        check_vma=False,
    )
```

```python
import functools

import jax
import jax.numpy as jnp
import numpy as np
from jax import lax
from jax.experimental import pallas as pl
from jax.experimental.pallas import tpu as pltpu
from jax.sharding import PartitionSpec as P


BLK = 64
NNZ = 2
MU_DEV = 128
CHUNKS = (2, 1, 1, 1)
SPARE = 2


SIGN_ENTRIES = (
    (0, 0, 0, 1),
    (0, 1, 1, 1),
    (0, 2, 2, 1),
    (0, 3, 3, 1),
    (1, 0, 1, -1),
    (1, 1, 0, 1),
    (1, 2, 3, -1),
    (1, 3, 2, 1),
    (2, 0, 2, -1),
    (2, 1, 3, 1),
    (2, 2, 0, 1),
    (2, 3, 1, -1),
    (3, 0, 3, -1),
    (3, 1, 2, -1),
    (3, 2, 1, 1),
    (3, 3, 0, 1),
)
F32 = jnp.float32
BF16 = jnp.bfloat16
LANES = 128
HEAD = 4


def mix_table():
    table = np.zeros((4, LANES, LANES), np.float32)
    for r, q, s, sign in SIGN_ENTRIES:
        for base in range(0, LANES, 4):
            table[r, base + s, base + q] = sign
    return table.reshape(4 * LANES, LANES)


def params(mebibytes=16):
    return pltpu.CompilerParams(vmem_limit_bytes=mebibytes * 1024 * 1024)


def picked_pair(info, tables, row, rows, width):
    tops, bottoms = [], []
    lane = lax.broadcasted_iota(jnp.int32, (BLK, LANES), 1)
    left = lane < width
    for k in range(NNZ):
        code = info[HEAD + k * rows + row]
        safe = jnp.maximum(code, 0)
        side = jnp.bitwise_and(safe, 1)
        block = jnp.right_shift(safe, 1)
        if len(tables) == 1:
            tile = tables[0][block].astype(F32)
        else:
            part = jnp.bitwise_and(block, 1)
            block = jnp.right_shift(block, 1)
            tile = jnp.where(part == 0, tables[0][block].astype(F32), tables[1][block].astype(F32))
        tile = jnp.where(code >= 0, tile, 0.0)
        other = jnp.concatenate([tile[:, width:], tile[:, :width]], axis=1)
        low = jnp.where(side == 0, tile, other)
        high = jnp.where(side == 0, other, tile)
        tops.append(jnp.where(left, low, 0.0).astype(BF16))
        bottoms.append(jnp.where(left, 0.0, high).astype(BF16))
    return jnp.concatenate(tops + bottoms, axis=0)


def half_rows(ints, right):
    count, blk, stored = ints.shape
    pairs = count // 2
    lhs = jnp.concatenate(
        [ints[:pairs].reshape(pairs * blk, stored), ints[pairs:].reshape(pairs * blk, stored)], axis=1
    )
    return jnp.dot(lhs, right, preferred_element_type=F32).astype(BF16)


def window_kernel(info, ints_ref, *rest, rows, width):
    *tables, out_ref = rest
    for rb in range(ints_ref.shape[1]):
        value = half_rows(ints_ref[:, rb], picked_pair(info, tables, rb, rows, width))
        for p in range(value.shape[0] // BLK):
            out_ref[rb * BLK : (rb + 1) * BLK, p * LANES : (p + 1) * LANES] = value[p * BLK : (p + 1) * BLK]


def half_kernel(info, a_ref, b_ref, *rest, rows, width, per, first, flip):
    *tables, a_out, b_out = rest
    x, y = jnp.bitwise_xor(info[0], flip), jnp.bitwise_xor(info[1], flip)
    step = first + pl.program_id(1)
    color_rows(info, a_ref, b_ref, tables, pl.program_id(0), step, x, y, rows, width, per, a_out, b_out)


def color_rows(info, a_ref, b_ref, tables, zl, step, x, y, rows, width, per, a_out, b_out):
    for other in range(2):
        for color, row in enumerate(
            (
                ((zl * 2 + other) * 2 + x) * per + step,
                ((zl * 2 + y) * 2 + other) * per + (per - SPARE) // 2 + step,
            )
        ):
            right = picked_pair(info, tables, row, rows, width)
            value = half_rows(b_ref[:, 0, 0, other, 0] if color else a_ref[:, 0, other, 0, 0], right)
            out = b_out if color else a_out
            for p in range(value.shape[0] // BLK):
                out[0, other, 0, :, p * LANES : (p + 1) * LANES] = value[p * BLK : (p + 1) * BLK]


def spare_kernel(info, ints_ref, *rest, rows, width, per):
    *tables, out_ref = rest
    zl, step = pl.program_id(0), pl.program_id(1)
    for plane in range(4):
        row = (zl * 4 + plane) * per + per - SPARE + step
        value = half_rows(ints_ref[:, 0, plane, 0], picked_pair(info, tables, row, rows, width))
        for p in range(value.shape[0] // BLK):
            out_ref[0, plane, 0, :, p * LANES : (p + 1) * LANES] = value[p * BLK : (p + 1) * BLK]


def half_call(info, ints7, tables, width, name, first=None, count=None):
    aux, zl, _, _, per, blk, stored = ints7.shape
    side = (per - SPARE) // 2
    flip, shift, steps = (0, 0, side) if first is None else (1, first, count)
    common = dict(rows=zl * 4 * per, width=width, per=per)
    if name == "half_spare":
        steps, planes = SPARE, 4
        kernel = functools.partial(spare_kernel, **common)
        operands = [ints7.reshape(aux, zl, 4, per, blk, stored)]
        inputs = [pl.BlockSpec((aux, 1, 4, 1, blk, stored), lambda i, j, s: (0, i, 0, per - SPARE + j, 0, 0))]
    else:
        planes = 2
        kernel = functools.partial(half_kernel, first=shift, flip=flip, **common)
        operands = [ints7] * 2
        inputs = [
            pl.BlockSpec(
                (aux, 1, 2, 1, 1, blk, stored), lambda i, j, s: (0, i, 0, jnp.bitwise_xor(s[0], flip), shift + j, 0, 0)
            ),
            pl.BlockSpec(
                (aux, 1, 1, 2, 1, blk, stored),
                lambda i, j, s: (0, i, jnp.bitwise_xor(s[1], flip), 0, side + shift + j, 0, 0),
            ),
        ]
    shape = jax.ShapeDtypeStruct((zl, planes, steps, blk, aux * width), BF16)
    spec = pl.BlockSpec((1, planes, 1, blk, aux * width), lambda i, j, s: (i, 0, j, 0, 0))
    work = 4 * zl * steps * aux * blk
    return pl.pallas_call(
        kernel,
        grid_spec=pltpu.PrefetchScalarGridSpec(
            num_scalar_prefetch=1,
            grid=(zl, steps),
            in_specs=inputs + [pl.BlockSpec(tables[0].shape, lambda i, j, s: (0, 0, 0))] * len(tables),
            out_specs=[spec] * len(inputs),
        ),
        out_shape=[shape] * len(inputs),
        compiler_params=params(40),
        cost_estimate=pl.CostEstimate(
            flops=work * stored * LANES * 8, bytes_accessed=work * (stored + width) * 2, transcendentals=0
        ),
    )(info, *operands, *tables)


def mix_kernel(info, table_ref, *rest, parts):
    *windows, out_ref = rest
    b = info[3]
    depth = out_ref.shape[2]
    for shift in range(parts):
        slot = lax.rem(b - shift + parts, parts)
        for t in range(depth // LANES):
            tile = windows[shift][0, :, t * LANES : (t + 1) * LANES]
            mixed = lax.dot_general(
                table_ref[...], tile, (((1,), (1,)), ((), ())), preferred_element_type=F32
            ).astype(BF16)
            for r in range(4):
                out_ref[0, slot, t * LANES : (t + 1) * LANES, r * MU_DEV : (r + 1) * MU_DEV] = mixed[
                    r * LANES : (r + 1) * LANES
                ]


def both_sums(refs, own_ref, mix_ref, place, count):
    a_own, b_own, a_got, b_got = refs[:count], refs[count : 2 * count], refs[2 * count], refs[2 * count + 1]
    zl, depth = a_own[0].shape[0], a_own[0].shape[4]
    rows = zl * count * BLK
    own = [ref[:, 0] for ref in a_own], [ref[:, 0] for ref in b_own]
    own = [jnp.concatenate(pieces, axis=1).reshape(rows, depth) for pieces in own]
    both = jnp.dot(jnp.concatenate(own, axis=0), own_ref[0, place], preferred_element_type=F32)
    sums = []
    for n, got in enumerate((a_got, b_got)):
        more = jnp.dot(got[...].reshape(rows, depth), mix_ref[n, place], preferred_element_type=F32)
        sums.append(both[n * rows : (n + 1) * rows] + more)
    return sums


def send_kernel(info, *refs, count):
    *refs, own_ref, mix_ref, a_out, b_out = refs
    cols = mix_ref.shape[3]
    for place in range(mix_ref.shape[1]):
        for total, out in zip(both_sums(refs, own_ref, mix_ref, place, count), (a_out, b_out)):
            out[:, :, :, place * cols : (place + 1) * cols] = total.astype(BF16).reshape(out.shape[:3] + (cols,))


def keep_kernel(info, *refs, count, hops):
    refs, outs = refs[:-hops], refs[-hops:]
    *refs, a_add, b_add, own_ref, mix_ref = refs
    parts, cols = mix_ref.shape[1], mix_ref.shape[3]
    zl = hops // parts
    for place in range(parts):
        sums = both_sums(refs, own_ref, mix_ref, place, count)
        for color, add in enumerate((a_add, b_add)):
            more = add[:, :, :, place * cols : (place + 1) * cols].astype(F32)
            sums[color] = (sums[color].reshape(more.shape) + more).astype(BF16)
        for group in range(zl):
            k = jnp.bitwise_xor(info[2], group * parts + place)
            for hop in range(hops):

                @pl.when(k == hop)
                def _(hop=hop, group=group, sums=sums):
                    for color in range(2):
                        outs[hop][color] = sums[color][group]


def spare_sums_kernel(info, half_ref, own_ref, *outs):
    zl, planes, count, blk, depth = half_ref.shape
    parts = own_ref.shape[1]
    for place in range(parts):
        for group in range(zl):
            total = jnp.dot(
                half_ref[group].reshape(planes * count * blk, depth), own_ref[0, place], preferred_element_type=F32
            )
            total = total.astype(BF16).reshape(outs[0].shape)
            k = jnp.bitwise_xor(info[2], group * parts + place)
            for hop, out in enumerate(outs):

                @pl.when(k == hop)
                def _(out=out, total=total):
                    out[...] = total


def add_all(refs, index):
    total = refs[0][index].astype(F32)
    for ref in refs[1:]:
        total += ref[index].astype(F32)
    return total


def plane_kernel(info, *refs, hops):
    got, (x_out, y_out, x_keep, y_keep) = refs[:hops], refs[hops:]
    x, y = info[0], info[1]
    for other in range(2):
        x_keep[other] = add_all(got, (other * 2 + x, 0))
        y_keep[other] = add_all(got, (y * 2 + other, 1))
        x_out[other] = add_all(got, (other * 2 + 1 - x, 0)).astype(BF16)
        y_out[other] = add_all(got, ((1 - y) * 2 + other, 1)).astype(BF16)


def line_kernel(info, x_keep, y_keep, x_got, y_got, y_out, x_out, first_keep, second_keep):
    x, y = info[0], info[1]
    first_keep[...] = add_all((x_keep, x_got), y)
    second_keep[...] = add_all((y_keep, y_got), x)
    y_out[...] = add_all((x_keep, x_got), 1 - y).astype(BF16)
    x_out[...] = add_all((y_keep, y_got), 1 - x).astype(BF16)


def simple_call(kernel, info, operands, outs, flops=0):
    def spec(value):
        return pl.BlockSpec(value.shape, lambda i, s, n=len(value.shape): (0,) * n)

    return pl.pallas_call(
        kernel,
        grid_spec=pltpu.PrefetchScalarGridSpec(
            num_scalar_prefetch=1, grid=(1,), in_specs=[spec(v) for v in operands], out_specs=[spec(o) for o in outs]
        ),
        out_shape=outs,
        compiler_params=params(),
        cost_estimate=pl.CostEstimate(flops=flops or 10**8, bytes_accessed=10**6, transcendentals=0),
    )(info, *operands)


def sums_call(info, keep, got, own_mix, mix, first, count, hops, adds=None):
    (a_keep, b_keep), (a_got, b_got) = keep, got
    zl, _, _, blk, depth = a_keep.shape
    _, parts, _, cols = mix.shape
    flip = 1 if adds is None else 0

    def own(axis):
        return [
            pl.BlockSpec((zl, 1, 1, blk, depth), lambda i, s, n=n: (0, jnp.bitwise_xor(s[axis], flip), first + n, 0, 0))
            for n in range(count)
        ]

    def other(axis):
        return [pl.BlockSpec((zl, 1, count, blk, depth), lambda i, s: (0, jnp.bitwise_xor(s[axis], flip), 0, 0, 0))]

    specs = own(1) + own(0) + other(1) + other(0)
    operands = [a_keep] * count + [b_keep] * count + [a_got, b_got]
    if adds is not None:
        specs += [pl.BlockSpec((zl, count, blk, parts * cols), lambda i, s: (0, 0, 0, 0))] * 2
        operands += list(adds)
    specs += [pl.BlockSpec(m.shape, lambda i, s: (0, 0, 0, 0)) for m in (own_mix, mix)]
    if adds is None:
        kernel = functools.partial(send_kernel, count=count)
        outs = [jax.ShapeDtypeStruct((zl, count, blk, parts * cols), BF16)] * 2
    else:
        kernel = functools.partial(keep_kernel, count=count, hops=hops)
        outs = [jax.ShapeDtypeStruct((2, count, blk, cols), BF16)] * hops
    return pl.pallas_call(
        kernel,
        grid_spec=pltpu.PrefetchScalarGridSpec(
            num_scalar_prefetch=1,
            grid=(1,),
            in_specs=specs,
            out_specs=[pl.BlockSpec(o.shape, lambda i, s: (0, 0, 0, 0)) for o in outs],
        ),
        out_shape=outs,
        compiler_params=params(),
        cost_estimate=pl.CostEstimate(
            flops=2 * 4 * zl * count * blk * depth * parts * cols,
            bytes_accessed=2 * (4 * zl * count * blk * depth + 3 * depth * parts * cols),
            transcendentals=0,
        ),
        name="send_sums" if adds is None else "keep_sums",
    )(info, *operands, own_mix, mix)


def final_kernel(*refs, starts, counts, hops):
    *refs, first_keep, second_keep, first_got, second_got, out_ref = refs
    per = out_ref.shape[0]
    half = (per - SPARE) // 2

    def store(row, total):
        for r in range(4):
            out_ref[row, :, r, :] = total[:, r * MU_DEV : (r + 1) * MU_DEV]

    for n, (first, count) in enumerate(zip(starts, counts)):
        for color in range(2):
            for rb in range(count):
                store(color * half + first + rb, add_all(refs[n * hops : (n + 1) * hops], (color, rb)))
    store(per - 2, add_all((first_keep, first_got), ...))
    store(per - 1, add_all((second_keep, second_got), ...))


def last_kernel(*refs, count, hops):
    out_ref = refs[-1]
    color = pl.program_id(0)
    for rb in range(count):
        total = refs[0][color, rb].astype(F32)
        for k in range(1, hops):
            total += refs[k][color, rb].astype(F32)
        for r in range(4):
            out_ref[rb, :, r, :] = total[:, r * MU_DEV : (r + 1) * MU_DEV]


def shards(ints, coeffs, offsets, mask, *, fit, parts):
    aux, rows, stored = ints.shape
    local, width = coeffs.shape
    hops = fit // 4
    zl = fit // (4 * parts)
    owned = local // BLK
    row_blocks = rows // BLK
    per = row_blocks // (4 * zl)
    half = owned // 2
    split = 2 if parts == 2 and half % 2 == 0 else 1

    f = lax.axis_index("fit").astype(jnp.int32)
    b = lax.axis_index("basis").astype(jnp.int32)
    x, y, z = f & 1, (f >> 1) & 1, f >> 2

    def over(pattern):
        return [(i, pattern(i)) for i in range(fit)]

    def hop_x(value):
        return lax.ppermute(value, "fit", over(lambda i: i ^ 1))

    def hop_y(value):
        return lax.ppermute(value, "fit", over(lambda i: i ^ 2))

    def across(value, shift):
        return lax.ppermute(value, "basis", [(i, (i + shift) % parts) for i in range(parts)])

    table = jnp.concatenate([coeffs[: local // 2], coeffs[local // 2 :]], axis=1)
    if split == 2:
        table = lax.dynamic_slice_in_dim(table, b * (local // 4), local // 4, 0)

    def spread(value, along):
        def goal(i, core, s):
            plane = along if split == 1 else along ^ (core == 1)
            return i ^ s if plane else i ^ (4 * s)

        return [
            lax.ppermute(
                value, ("fit", "basis"), [(i * parts + c, goal(i, c, s) * parts + c) for i in range(fit) for c in range(parts)]
            )
            for s in range(1, hops)
        ]

    even = hops == 4
    if even:
        table = jnp.stack([table] + spread(table, False))
        table = jnp.stack([table] + spread(table, True))
    else:
        table = lax.all_gather(table, "fit", axis=0)
    tables = [table.reshape(-1, BLK, 2 * width)]
    if split == 2:
        tables.append(across(tables[0], 1))

    source, inner = offsets // owned, offsets % owned
    side, inner = inner // half, inner % half
    share = half // split
    near, far = (source & 3) ^ (f & 3), (source >> 2) ^ z
    if not even:
        code = source
    elif split == 2:
        code = jnp.where(inner // share == 0, near * hops + far, far * 4 + near)
    else:
        code = near * hops + far
    code = code * share + inner % share
    if split == 2:
        code = code * 2 + ((inner // share) ^ b)
    code = jnp.where(mask != 0, code * 2 + side, -1)
    info = jnp.concatenate([jnp.stack([x, y, z, b]), code.T.reshape(-1)])

    ints7 = ints.reshape(aux, zl, 2, 2, per, BLK, stored)
    depth = aux * width
    whole = pl.BlockSpec(memory_space=pltpu.VMEM)
    window_blocks = MU_DEV // BLK
    window_call = pl.pallas_call(
        functools.partial(window_kernel, rows=row_blocks, width=width),
        grid_spec=pltpu.PrefetchScalarGridSpec(
            num_scalar_prefetch=1,
            grid=(1,),
            in_specs=[pl.BlockSpec((aux, window_blocks, BLK, stored), lambda i, s: (0, 0, 0, 0))]
            + [pl.BlockSpec(tables[0].shape, lambda i, s: (0, 0, 0))] * len(tables),
            out_specs=pl.BlockSpec((MU_DEV, depth), lambda i, s: (0, 0)),
        ),
        out_shape=jax.ShapeDtypeStruct((MU_DEV, depth), BF16),
        compiler_params=params(40),
        cost_estimate=pl.CostEstimate(
            flops=2 * MU_DEV * depth * stored, bytes_accessed=2 * MU_DEV * depth * 4, transcendentals=0
        ),
        name="window",
    )
    window = window_call(info, ints.reshape(aux, row_blocks, BLK, stored), *tables)
    wx, wy = hop_x(window), hop_y(window)

    firsts = [sum(CHUNKS[:n]) for n in range(len(CHUNKS))]
    counts = list(CHUNKS)
    sends = [half_call(info, ints7, tables, width, f"half_{n}", firsts[n], counts[n]) for n in range(len(counts))]
    gots = [(hop_x(a), hop_y(b)) for a, b in sends]
    (spare,) = half_call(info, ints7, tables, width, "half_spare")
    a_keep, b_keep = half_call(info, ints7, tables, width, "half_keep")

    cols = 4 * MU_DEV

    def mixed(values):
        stack = jnp.stack(values)
        stacks = [stack] + [across(stack, s) for s in range(1, parts)]
        return pl.pallas_call(
            functools.partial(mix_kernel, parts=parts),
            grid_spec=pltpu.PrefetchScalarGridSpec(
                num_scalar_prefetch=1,
                grid=(len(values),),
                in_specs=[pl.BlockSpec((4 * LANES, LANES), lambda i, s: (0, 0))]
                + [pl.BlockSpec((1, MU_DEV, depth), lambda i, s: (i, 0, 0))] * parts,
                out_specs=pl.BlockSpec((1, parts, depth, cols), lambda i, s: (i, 0, 0, 0)),
            ),
            out_shape=jax.ShapeDtypeStruct((len(values), parts, depth, cols), BF16),
            compiler_params=params(),
            cost_estimate=pl.CostEstimate(
                flops=2 * len(values) * parts * depth * cols * LANES,
                bytes_accessed=2 * len(values) * parts * depth * cols,
                transcendentals=0,
            ),
        )(info, jnp.asarray(mix_table(), BF16), *stacks)

    own_mix = mixed([window])
    mix = mixed([wx, wy])

    def along_z(values):
        moved = []
        for k, value in enumerate(values):
            pairs = []
            for i in range(fit):
                for core in range(parts):
                    goal = core * hops + ((i >> 2) ^ k)
                    pairs.append((i * parts + core, ((goal // parts) * 4 + (i & 3)) * parts + goal % parts))
            moved.append(lax.ppermute(value, ("fit", "basis"), pairs))
        return moved

    def shaped(shape, kind):
        return jax.ShapeDtypeStruct(shape, kind)

    outs = [shaped((4, SPARE, BLK, cols), BF16)] * hops
    flops = 2 * zl * 4 * SPARE * BLK * depth * parts * cols
    spares = along_z(simple_call(spare_sums_kernel, info, [spare, own_mix], outs, flops))
    outs = [shaped((2, BLK, cols), BF16)] * 2 + [shaped((2, BLK, cols), F32)] * 2
    x_sum, y_sum, x_keep, y_keep = simple_call(functools.partial(plane_kernel, hops=hops), info, spares, outs)
    x_sum, y_sum = hop_x(x_sum), hop_y(y_sum)
    outs = [shaped((BLK, cols), BF16)] * 2 + [shaped((BLK, cols), F32)] * 2
    first_sum, second_sum, *spare_keep = simple_call(line_kernel, info, [x_keep, y_keep, x_sum, y_sum], outs)
    spare_got = [hop_y(first_sum), hop_x(second_sum)]

    final = []
    for n, got in enumerate(gots):
        a_sum, b_sum = sums_call(info, (a_keep, b_keep), got, own_mix, mix, firsts[n], counts[n], hops)
        adds = hop_y(a_sum), hop_x(b_sum)
        outs = sums_call(info, (a_keep, b_keep), got, own_mix, mix, firsts[n], counts[n], hops, adds)
        final += along_z(outs)

    shape = jax.ShapeDtypeStruct((per, BLK, 4, MU_DEV), F32)
    early = pl.pallas_call(
        functools.partial(final_kernel, starts=firsts[:-1], counts=counts[:-1], hops=hops),
        in_specs=[whole] * (len(final[:-hops]) + 4),
        out_specs=whole,
        out_shape=shape,
        compiler_params=params(),
        cost_estimate=pl.CostEstimate(
            flops=hops * per * BLK * cols, bytes_accessed=(2 * hops + 4) * per * BLK * cols, transcendentals=0
        ),
        name="early",
    )(*final[:-hops], *spare_keep, *spare_got)
    last = counts[-1]
    result = pl.pallas_call(
        functools.partial(last_kernel, count=last, hops=hops),
        grid=(2,),
        in_specs=[pl.BlockSpec(final[-1].shape, lambda i: (0, 0, 0, 0))] * hops + [pl.BlockSpec(memory_space=pl.ANY)],
        out_specs=pl.BlockSpec((last, BLK, 4, MU_DEV), lambda i: ((i + 1) * ((per - SPARE) // (2 * last)) - 1, 0, 0, 0)),
        out_shape=shape,
        input_output_aliases={hops: 0},
        compiler_params=params(),
        name="last",
    )(*final[-hops:], early)
    result = result.reshape(per * BLK, 4, MU_DEV)
    if lax.axis_size("occ") > 1:
        result = lax.psum_scatter(result, "occ", scatter_dimension=0, tiled=True)
    return result


def solution(mesh):
    def body(*args):
        return shards(*args, fit=mesh.shape["fit"], parts=mesh.shape["basis"])

    return jax.shard_map(
        body,
        mesh=mesh,
        in_specs=(P("fit", "basis", None), P("fit", "occ"), P("basis", None), P("basis", None)),
        out_specs=P(("fit", "occ"), None, "basis"),
        check_vma=False,
    )
```
